512 devices in a mesh: seq: 64 (over z, x_lo, core), tp: 8 (over x_hi, y).
Axes of the slice: x: 4 (x_hi: 2, x_lo: 2; x = x_hi * 2 + x_lo), y: 4, z: 16, core: 2. Of those that a mesh axis runs over, the one named last changes fastest.
Arguments:
- tokens: bfloat16 [32768, 3584], P(('seq', 'tp')), may hold values from -6 to 6
- pre_gain: float32 [3584], replicated, may hold values from 0.25 to 1.75
- post_gain: float32 [3584], replicated, may hold values from 0.25 to 1.75
- w_query: bfloat16 [3584, 4096], P('seq', 'tp'), may hold values from -0.09375 to 0.09375
- key_matrix: bfloat16 [3584, 2048], P('seq', 'tp'), may hold values from -0.09375 to 0.09375
- value_matrix: bfloat16 [3584, 2048], P('seq', 'tp'), may hold values from -0.09375 to 0.09375
- w_out: bfloat16 [4096, 3584], P('tp', 'seq'), may hold values from -0.09375 to 0.09375
Outputs:
- block_out: bfloat16 [32768, 3584], P(('seq', 'tp'))
The draws below stay inside these ranges and needn't reach their ends.
All inputs are finite; a program needn't handle non-finite values.
Results may differ from the reference program's by a relative error of at most 0.014.
Values may be sent and summed in bfloat16 or wider, within the bound.
No kernel may reach another device: no remote copies, remote signals or barrier semaphores. Data moves between devices by JAX's collectives and lax.ppermute only.
A program may use at most 64 MiB of HBM per device.

```python
import jax
import jax.numpy as jnp
from jax import lax

MODEL_WIDTH = 3584
QUERY_HEADS = 16
KEY_VALUE_HEADS = 8
HEAD_SIZE = 256
BLOCK_TOKENS = 512
TOKENS = 32768
N_SEQ = 64
N_TP = 8


def shard_levels(rng, shape, split, least, largest):
    def one(axis_at, blocks):
        steps = jax.random.uniform(jax.random.fold_in(jax.random.fold_in(rng, 6), axis_at), (blocks,), jnp.float32, least / len(split), largest / len(split))
        return jnp.repeat(jnp.exp(steps), shape[axis_at] // blocks).reshape((-1,) + (1,) * (len(shape) - axis_at - 1))

    factor_of = one(*split[0])
    for cut in split[1:]:
        factor_of = factor_of * one(*cut)
    return factor_of


def scatter_about(key, shape, deviation, limit, shards=(), held_as=jnp.bfloat16):
    result = jax.random.normal(key, shape, jnp.float32) * deviation
    if len(shards) > 0:
        result = shard_levels(key, shape, shards, -0.22, 0.18) * result
    return jnp.clip(result, min=-limit, max=limit).astype(held_as)


def setup_inputs(seed: int = 0) -> dict:
    splits = jax.random.split(jax.random.key(seed), 8)
    return {
        "tokens": scatter_about(splits[0], (TOKENS, MODEL_WIDTH), 1.0, 6.0, ((0, 512),)),
        "pre_gain": jnp.clip(1.0 + 0.15 * jax.random.normal(splits[1], (MODEL_WIDTH,), jnp.float32), 0.25, 1.75),
        "post_gain": jnp.clip(1.0 + 0.15 * jax.random.normal(splits[2], (MODEL_WIDTH,), jnp.float32), 0.25, 1.75),
        "w_query": scatter_about(splits[3], (MODEL_WIDTH, QUERY_HEADS * HEAD_SIZE), MODEL_WIDTH ** -0.5, 0.09375, ((0, 64), (1, 8))),
        "key_matrix": scatter_about(splits[4], (MODEL_WIDTH, KEY_VALUE_HEADS * HEAD_SIZE), MODEL_WIDTH ** -0.5, 0.09375, ((0, 64), (1, 8))),
        "value_matrix": scatter_about(splits[5], (MODEL_WIDTH, KEY_VALUE_HEADS * HEAD_SIZE), MODEL_WIDTH ** -0.5, 0.09375, ((0, 64), (1, 8))),
        "w_out": scatter_about(splits[6], (QUERY_HEADS * HEAD_SIZE, MODEL_WIDTH), (QUERY_HEADS * HEAD_SIZE) ** -0.5, 0.09375, ((0, 8), (1, 64))),
    }


def root_norm(values, gain):
    values = values.astype(jnp.float32)
    return values * lax.rsqrt(lax.optimization_barrier(jnp.mean(values * values, axis=-1, keepdims=True)) + 1e-06) * gain.astype(jnp.float32)

def rotate_halves(values, token_positions):
    row_count = values.shape[0]
    shaped = values.reshape(row_count, -1, HEAD_SIZE)
    half_dim = HEAD_SIZE // 2
    freq = 10000.0 ** (-(jnp.arange(half_dim).astype(jnp.float32) * 2.0 / HEAD_SIZE))
    angle = token_positions[:, None] * freq[None, :]
    cosine = jnp.cos(angle)[:, None, :]
    sine_part = jnp.sin(angle)[:, None, :]
    first = shaped[..., :half_dim]
    second = shaped[..., half_dim:]
    turned = jnp.concatenate([first * cosine - second * sine_part, second * cosine + first * sine_part], axis=-1)
    return turned.reshape(row_count, -1)

def reference(tokens, pre_gain, post_gain, w_query, key_matrix, value_matrix, w_out):
    repeat_heads = QUERY_HEADS // KEY_VALUE_HEADS
    normalized_input = root_norm(tokens, pre_gain).astype(jnp.bfloat16)
    token_positions = jnp.arange(TOKENS).astype(jnp.float32)
    key_window = jnp.dot(normalized_input, key_matrix, preferred_element_type=jnp.float32)
    key_window = rotate_halves(key_window, token_positions).astype(jnp.bfloat16).reshape(N_SEQ, BLOCK_TOKENS, KEY_VALUE_HEADS, HEAD_SIZE)
    value_window = jnp.dot(normalized_input, value_matrix, preferred_element_type=jnp.float32).astype(jnp.bfloat16).reshape(N_SEQ, BLOCK_TOKENS, KEY_VALUE_HEADS, HEAD_SIZE)
    blank_rows = jnp.zeros((1, BLOCK_TOKENS, KEY_VALUE_HEADS, HEAD_SIZE), jnp.bfloat16)
    keys_prior = jnp.concatenate([blank_rows, key_window[:-1]], axis=0)
    vals_prior = jnp.concatenate([blank_rows, value_window[:-1]], axis=0)
    normed_blocks = normalized_input.reshape(N_SEQ, BLOCK_TOKENS, MODEL_WIDTH)
    token_blocks = tokens.reshape(N_SEQ, BLOCK_TOKENS, MODEL_WIDTH)
    out_groups = w_out.astype(jnp.float32).reshape(N_TP, QUERY_HEADS * HEAD_SIZE // N_TP, MODEL_WIDTH)

    def one_block(block_index):
        rows = normed_blocks[block_index]
        offset_pos = block_index * BLOCK_TOKENS
        local_pos = (offset_pos + jnp.arange(BLOCK_TOKENS).astype(jnp.int32)).astype(jnp.float32)
        raw_q = jnp.dot(rows, w_query, preferred_element_type=jnp.float32)
        query_rows = (rotate_halves(raw_q, local_pos) * HEAD_SIZE ** (-0.5)).astype(jnp.bfloat16)
        query_rows = query_rows.reshape(BLOCK_TOKENS, KEY_VALUE_HEADS, repeat_heads, HEAD_SIZE).astype(jnp.float32)
        key_current = jnp.concatenate([keys_prior[block_index], key_window[block_index]], axis=0).astype(jnp.float32)
        value_current = jnp.concatenate([vals_prior[block_index], value_window[block_index]], axis=0).astype(jnp.float32)
        attention_scores = jnp.einsum('cwap,bwp->wacb', query_rows, key_current)
        query_idx = jnp.arange(BLOCK_TOKENS).astype(jnp.int32)[:, None]
        key_idx = jnp.arange(2 * BLOCK_TOKENS).astype(jnp.int32)[None, :]
        key_pos = offset_pos - BLOCK_TOKENS + key_idx
        allowed = (key_idx > query_idx) & (key_idx <= query_idx + BLOCK_TOKENS) & (key_pos >= 0)
        weights = jnp.where(allowed, jnp.exp(attention_scores), 0.0)
        denominator = lax.optimization_barrier(jnp.sum(weights, axis=-1))
        weight_narrow = weights.astype(jnp.bfloat16).astype(jnp.float32)
        reduced_output = jnp.einsum('bpqu,ubm->qbpm', weight_narrow, value_current)
        attended = (reduced_output / jnp.transpose(denominator, (2, 0, 1))[..., None]).astype(jnp.bfloat16)
        attended = attended.reshape(BLOCK_TOKENS, N_TP, QUERY_HEADS * HEAD_SIZE // N_TP).astype(jnp.float32)
        partial_value = jnp.einsum('tgc,gcd->gtd', attended, out_groups).astype(jnp.bfloat16)
        partial_value = lax.optimization_barrier(partial_value)
        projected = lax.optimization_barrier(jnp.sum(partial_value.astype(jnp.float32), axis=0))
        mixed = root_norm(projected, post_gain)
        return (token_blocks[block_index].astype(jnp.float32) + mixed).astype(jnp.bfloat16)
    outputs = lax.map(one_block, jnp.arange(N_SEQ).astype(jnp.int32))
    return outputs.reshape(TOKENS, MODEL_WIDTH)
```

```python
import jax
import jax.numpy as jnp
from jax import lax
from jax.sharding import Mesh
from jax.sharding import PartitionSpec as P

HEAD_SIZE = 256
BLOCK_TOKENS = 512
SEQ = ("seq_0", "seq_1", "seq_2")
TP = ("tp_0", "tp_1")
SEQ_TP = ("seq_0", "seq_1", "seq_2", "tp_0", "tp_1")


def to_every_tp(x):
    length = lax.axis_size(TP)
    return lax.all_to_all(jnp.broadcast_to(x[None], (length, *x.shape)), TP, 0, 0, tiled=True)


def weights_of_heads(slab):
    pair = ("seq_1", "seq_2")
    first = lax.ppermute(slab, pair, [(1, 0), (0, 2), (3, 1), (2, 3)])
    second = lax.ppermute(slab, pair, [(1, 2), (2, 1)])
    chip, core = lax.axis_index("seq_1"), lax.axis_index("seq_2")
    same = chip == core
    upper = jnp.where(same, jnp.where(core == 0, slab, first), jnp.where(core == 0, first, second))
    lower = jnp.where(same, jnp.where(core == 0, first, slab), jnp.where(core == 0, second, first))
    mine = jnp.concatenate([upper, lower], axis=0)
    return lax.all_gather(mine, ("seq_0", "seq_2"), axis=0, tiled=True)


def from_behind(x, axis, by):
    length = lax.axis_size(axis)
    pairs = [(i, i + by) for i in range(length) if 0 <= i + by < length]
    return lax.ppermute(x, axis, pairs)


def root_norm(values, gain):
    values = values.astype(jnp.float32)
    return values * lax.rsqrt(jnp.mean(values * values, axis=-1, keepdims=True) + 1e-06) * gain


def rotate_halves(values, token_positions):
    row_count = values.shape[0]
    shaped = values.reshape(row_count, -1, HEAD_SIZE)
    half_dim = HEAD_SIZE // 2
    freq = 10000.0 ** (-(jnp.arange(half_dim).astype(jnp.float32) * 2.0 / HEAD_SIZE))
    angle = token_positions[:, None] * freq[None, :]
    cosine = jnp.cos(angle)[:, None, :]
    sine_part = jnp.sin(angle)[:, None, :]
    first = shaped[..., :half_dim]
    second = shaped[..., half_dim:]
    turned = jnp.concatenate(
        [first * cosine - second * sine_part, second * cosine + first * sine_part], axis=-1
    )
    return turned.reshape(row_count, -1)


def attend(query_rows, keys_now, vals_now, keys_prior, vals_prior, offset_pos):
    length = query_rows.shape[0]
    kv_heads = keys_now.shape[1] // HEAD_SIZE
    repeat_heads = query_rows.shape[1] // (HEAD_SIZE * kv_heads)
    query_grouped = query_rows.reshape(length, kv_heads, repeat_heads, HEAD_SIZE)
    key_current = jnp.concatenate([keys_prior, keys_now], axis=0).reshape(
        2 * length, kv_heads, HEAD_SIZE
    )
    value_current = jnp.concatenate([vals_prior, vals_now], axis=0).reshape(
        2 * length, kv_heads, HEAD_SIZE
    )
    attention_scores = jnp.einsum(
        "cwap,bwp->wacb", query_grouped, key_current, preferred_element_type=jnp.float32
    )
    query_idx = jnp.arange(length)[:, None]
    key_idx = jnp.arange(2 * length)[None, :]
    key_pos = offset_pos - length + key_idx
    allowed = (key_idx > query_idx) & (key_idx <= query_idx + length) & (key_pos >= 0)
    weights = jnp.where(allowed, jnp.exp(attention_scores), 0.0)
    denominator = jnp.sum(weights, axis=-1)
    weight_narrow = weights.astype(jnp.bfloat16)
    reduced_output = jnp.einsum(
        "bpqu,ubm->qbpm", weight_narrow, value_current, preferred_element_type=jnp.float32
    )
    attended = reduced_output / jnp.transpose(denominator, (2, 0, 1))[..., None]
    return attended.astype(jnp.bfloat16).reshape(length, -1)


def local(tokens, pre_gain, post_gain, w_query, key_matrix, value_matrix, w_out):
    normalized_input = root_norm(tokens, pre_gain).astype(jnp.bfloat16)
    query_cols = w_query.shape[1]
    key_cols = key_matrix.shape[1]
    slab = jnp.concatenate([w_query, key_matrix, value_matrix, w_out.T], axis=1)
    gathered = weights_of_heads(slab)
    width = query_cols + 2 * key_cols
    piece = to_every_tp(normalized_input).reshape(-1, normalized_input.shape[1])
    joined = jnp.dot(piece, gathered[:, :width], preferred_element_type=jnp.float32)
    raw_q = joined[:, :query_cols]
    raw_k = joined[:, query_cols : query_cols + key_cols]
    raw_v = joined[:, query_cols + key_cols :]
    offset_pos = lax.axis_index(SEQ) * BLOCK_TOKENS
    token_positions = (offset_pos + jnp.arange(BLOCK_TOKENS)).astype(jnp.float32)
    query_rows = (rotate_halves(raw_q, token_positions) * HEAD_SIZE ** (-0.5)).astype(jnp.bfloat16)
    keys_now = rotate_halves(raw_k, token_positions).astype(jnp.bfloat16)
    vals_now = raw_v.astype(jnp.bfloat16)
    keys_prior, vals_prior = from_behind((keys_now, vals_now), SEQ, 1)
    attended = attend(query_rows, keys_now, vals_now, keys_prior, vals_prior, offset_pos)
    partial_value = lax.dot_general(
        attended, gathered[:, width:], (((1,), (1,)), ((), ())), preferred_element_type=jnp.float32
    )
    length = lax.axis_size(TP)
    pieces = partial_value.astype(jnp.bfloat16).reshape(length, -1, partial_value.shape[1])
    received = lax.all_to_all(pieces, TP, 0, 0, tiled=True)
    own_rows = jnp.sum(received.astype(jnp.float32), axis=0)
    mixed = root_norm(own_rows, post_gain)
    return (tokens.astype(jnp.float32) + mixed).astype(jnp.bfloat16)


def solution(mesh):
    finer = Mesh(mesh.devices.reshape(16, 2, 2, 2, 4), ("seq_0", "seq_1", "seq_2", "tp_0", "tp_1"))
    in_specs = (P(SEQ_TP, None), P(), P(), P(SEQ, TP), P(SEQ, TP), P(SEQ, TP), P(TP, SEQ))
    out_specs = P(SEQ_TP, None)
    return jax.shard_map(local, mesh=finer, in_specs=in_specs, out_specs=out_specs, check_vma=False)
```

```python
import jax
import jax.numpy as jnp
from jax import lax
from jax.sharding import Mesh
from jax.sharding import PartitionSpec as P

HEAD_SIZE = 256
BLOCK_TOKENS = 512
SEQ = ("seq_0", "seq_1", "seq_2")
TP = ("tp_0", "tp_1")
SEQ_TP = ("seq_0", "seq_1", "seq_2", "tp_0", "tp_1")


def to_every_tp(x):
    length = lax.axis_size(TP)
    return lax.all_to_all(jnp.broadcast_to(x[None], (length, *x.shape)), TP, 0, 0, tiled=True)


def around(length, by):
    return [(i, (i + by) % length) for i in range(length)]


def chip_pair_block(slab):
    pair = ("seq_1", "seq_2")
    chip, core = lax.axis_index("seq_1"), lax.axis_index("seq_2")
    held = [slab] + [lax.ppermute(slab, pair, [(i, i ^ flip) for i in range(4)]) for flip in (1, 2, 3)]
    place = chip * 2 + core
    rows = []
    for k in range(4):
        flip = place ^ k
        rows.append(
            jnp.where(
                flip < 2, jnp.where(flip == 0, held[0], held[1]), jnp.where(flip == 2, held[2], held[3])
            )
        )
    return [jnp.concatenate(rows[:2], axis=0), jnp.concatenate(rows[2:], axis=0)]


def weights_of_heads(slab):
    length = lax.axis_size("seq_0")
    z, core = lax.axis_index("seq_0"), lax.axis_index("seq_2")
    step = jnp.where(core == 0, -1, 1)
    onward = [(2 * i + c, 2 * ((i + (1, -1)[c]) % length) + c) for i in range(length) for c in range(2)]
    streams = chip_pair_block(slab)
    whole = jnp.zeros((length, 2, *streams[0].shape), slab.dtype)

    def put(whole, blocks, at):
        return lax.dynamic_update_slice(whole, jnp.stack(blocks)[None], (at % length, 0, 0, 0))

    whole = put(whole, streams, z)
    half = length // 2
    waiting = []
    for k in range(1, half):
        streams = [lax.ppermute(s, ("seq_0", "seq_2"), onward) for s in streams]
        whole = put(whole, streams, z + step * k)
        waiting.append((k, jnp.stack(streams)))
        if k % 3 == 0:
            whole = swapped(whole, waiting, z, step, put)
            waiting = []
    last = lax.ppermute(jnp.where(core == 0, streams[0], streams[1]), ("seq_0", "seq_2"), onward)
    waiting.append((half, last[None]))
    return swapped(whole, waiting, z, step, put, last, core).reshape(-1, slab.shape[1])


def swapped(whole, waiting, z, step, put, last=None, core=None):
    sent = jnp.concatenate([b for _, b in waiting], axis=0)
    got = lax.ppermute(sent, "seq_2", around(2, 1))
    at = 0
    for k, blocks in waiting:
        if blocks.shape[0] == 2:
            whole = put(whole, [got[at], got[at + 1]], z - step * k)
        else:
            first = jnp.where(core == 0, last, got[at])
            second = jnp.where(core == 0, got[at], last)
            whole = put(whole, [first, second], z + k)
        at += blocks.shape[0]
    return whole


def from_behind(x, axis, by):
    length = lax.axis_size(axis)
    pairs = [(i, i + by) for i in range(length) if 0 <= i + by < length]
    return lax.ppermute(x, axis, pairs)


def root_norm(values, gain):
    values = values.astype(jnp.float32)
    return values * lax.rsqrt(jnp.mean(values * values, axis=-1, keepdims=True) + 1e-06) * gain


def rotate_halves(values, token_positions):
    row_count = values.shape[0]
    shaped = values.reshape(row_count, -1, HEAD_SIZE)
    half_dim = HEAD_SIZE // 2
    freq = 10000.0 ** (-(jnp.arange(half_dim).astype(jnp.float32) * 2.0 / HEAD_SIZE))
    angle = token_positions[:, None] * freq[None, :]
    cosine = jnp.cos(angle)[:, None, :]
    sine_part = jnp.sin(angle)[:, None, :]
    first = shaped[..., :half_dim]
    second = shaped[..., half_dim:]
    turned = jnp.concatenate(
        [first * cosine - second * sine_part, second * cosine + first * sine_part], axis=-1
    )
    return turned.reshape(row_count, -1)


def attend(query_rows, keys_now, vals_now, keys_prior, vals_prior, offset_pos):
    length = query_rows.shape[0]
    kv_heads = keys_now.shape[1] // HEAD_SIZE
    repeat_heads = query_rows.shape[1] // (HEAD_SIZE * kv_heads)
    query_grouped = query_rows.reshape(length, kv_heads, repeat_heads, HEAD_SIZE)
    key_current = jnp.concatenate([keys_prior, keys_now], axis=0).reshape(
        2 * length, kv_heads, HEAD_SIZE
    )
    value_current = jnp.concatenate([vals_prior, vals_now], axis=0).reshape(
        2 * length, kv_heads, HEAD_SIZE
    )
    attention_scores = jnp.einsum(
        "cwap,bwp->wacb", query_grouped, key_current, preferred_element_type=jnp.float32
    )
    query_idx = jnp.arange(length)[:, None]
    key_idx = jnp.arange(2 * length)[None, :]
    key_pos = offset_pos - length + key_idx
    allowed = (key_idx > query_idx) & (key_idx <= query_idx + length) & (key_pos >= 0)
    weights = jnp.where(allowed, jnp.exp(attention_scores), 0.0)
    denominator = jnp.sum(weights, axis=-1)
    weight_narrow = weights.astype(jnp.bfloat16)
    reduced_output = jnp.einsum(
        "bpqu,ubm->qbpm", weight_narrow, value_current, preferred_element_type=jnp.float32
    )
    attended = reduced_output / jnp.transpose(denominator, (2, 0, 1))[..., None]
    return attended.astype(jnp.bfloat16).reshape(length, -1)


def local(tokens, pre_gain, post_gain, w_query, key_matrix, value_matrix, w_out):
    normalized_input = root_norm(tokens, pre_gain).astype(jnp.bfloat16)
    query_cols = w_query.shape[1]
    key_cols = key_matrix.shape[1]
    slab = jnp.concatenate([w_query, key_matrix, value_matrix, w_out.T], axis=1)
    gathered = weights_of_heads(slab)
    width = query_cols + 2 * key_cols
    piece = to_every_tp(normalized_input).reshape(-1, normalized_input.shape[1])
    joined = jnp.dot(piece, gathered[:, :width], preferred_element_type=jnp.float32)
    raw_q = joined[:, :query_cols]
    raw_k = joined[:, query_cols : query_cols + key_cols]
    raw_v = joined[:, query_cols + key_cols :]
    offset_pos = lax.axis_index(SEQ) * BLOCK_TOKENS
    token_positions = (offset_pos + jnp.arange(BLOCK_TOKENS)).astype(jnp.float32)
    query_rows = (rotate_halves(raw_q, token_positions) * HEAD_SIZE ** (-0.5)).astype(jnp.bfloat16)
    keys_now = rotate_halves(raw_k, token_positions).astype(jnp.bfloat16)
    vals_now = raw_v.astype(jnp.bfloat16)
    keys_prior, vals_prior = from_behind((keys_now, vals_now), SEQ, 1)
    attended = attend(query_rows, keys_now, vals_now, keys_prior, vals_prior, offset_pos)
    partial_value = lax.dot_general(
        attended, gathered[:, width:], (((1,), (1,)), ((), ())), preferred_element_type=jnp.float32
    )
    length = lax.axis_size(TP)
    pieces = partial_value.astype(jnp.bfloat16).reshape(length, -1, partial_value.shape[1])
    received = lax.all_to_all(pieces, TP, 0, 0, tiled=True)
    own_rows = jnp.sum(received.astype(jnp.float32), axis=0)
    mixed = root_norm(own_rows, post_gain)
    return (tokens.astype(jnp.float32) + mixed).astype(jnp.bfloat16)


def solution(mesh):
    finer = Mesh(mesh.devices.reshape(16, 2, 2, 2, 4), ("seq_0", "seq_1", "seq_2", "tp_0", "tp_1"))
    in_specs = (P(SEQ_TP, None), P(), P(), P(SEQ, TP), P(SEQ, TP), P(SEQ, TP), P(TP, SEQ))
    out_specs = P(SEQ_TP, None)
    return jax.shard_map(local, mesh=finer, in_specs=in_specs, out_specs=out_specs, check_vma=False)
```

```python
import jax
import jax.numpy as jnp
from jax import lax
from jax.sharding import Mesh
from jax.sharding import PartitionSpec as P

HEAD_SIZE = 256
BLOCK_TOKENS = 512
SEQ = ("seq_0", "seq_1", "seq_2")
TP = ("tp_0", "tp_1")
SEQ_TP = ("seq_0", "seq_1", "seq_2", "tp_0", "tp_1")


def to_every_tp(x):
    length = lax.axis_size(TP)
    return lax.all_to_all(jnp.broadcast_to(x[None], (length, *x.shape)), TP, 0, 0, tiled=True)


def w_out_of_heads(slab):
    pair = ("seq_1", "seq_2")
    first = lax.ppermute(slab, pair, [(1, 0), (0, 2), (3, 1), (2, 3)])
    second = lax.ppermute(slab, pair, [(1, 2), (2, 1)])
    chip, core = lax.axis_index("seq_1"), lax.axis_index("seq_2")
    same = chip == core
    upper = jnp.where(same, jnp.where(core == 0, slab, first), jnp.where(core == 0, first, second))
    lower = jnp.where(same, jnp.where(core == 0, first, slab), jnp.where(core == 0, second, first))
    mine = jnp.concatenate([upper, lower], axis=0)
    return lax.all_gather(mine, ("seq_0", "seq_2"), axis=0, tiled=True)


def around(length, by):
    return [(i, (i + by) % length) for i in range(length)]


def ring_order(length):
    half = length // 2
    return [0] + [s * k for k in range(1, half) for s in (-1, 1)] + [half]


def in_ring_order(x):
    z, core = lax.axis_index("seq_0"), lax.axis_index("seq_2")
    length = lax.axis_size("seq_0")
    rows = x.shape[0]
    split = jnp.moveaxis(x.reshape(rows, length, 2, 2, -1), 0, 3)
    twice = jnp.concatenate([split, split], axis=0)
    turned = lax.dynamic_slice_in_dim(twice, z, length, axis=0)
    turned = jnp.stack([turned[o % length] for o in ring_order(length)])
    even, odd = turned[:, :, 0], turned[:, :, 1]
    own = jnp.where(core == 0, even, odd)
    other = jnp.where(core == 0, odd, even)
    both = jnp.stack([own, other])
    return jnp.moveaxis(both, 3, 0).reshape(rows, -1)


def ring_blocks(slab):
    length = lax.axis_size("seq_0")
    half = length // 2
    beside = lax.ppermute(slab, "seq_1", around(2, 1))
    chip = lax.axis_index("seq_1")
    own = jnp.concatenate([jnp.where(chip == 0, slab, beside), jnp.where(chip == 0, beside, slab)], axis=0)
    blocks = [own]
    up = down = own
    for _ in range(1, half):
        up = lax.ppermute(up, "seq_0", around(length, 1))
        down = lax.ppermute(down, "seq_0", around(length, -1))
        blocks += [up, down]
    rows = slab.shape[0]
    blocks += [lax.ppermute(up[:rows], "seq_0", around(length, 1)), lax.ppermute(down[rows:], "seq_0", around(length, -1))]
    return [jnp.concatenate(blocks[:half], axis=0), jnp.concatenate(blocks[half:], axis=0)]


def times_ring_weights(piece, slab):
    own = ring_blocks(slab)
    other = [lax.ppermute(b, "seq_2", around(2, 1)) for b in own]
    depth = own[0].shape[0]
    total = 0.0
    for k, block in enumerate(own + other):
        total = total + jnp.dot(piece[:, k * depth : (k + 1) * depth], block, preferred_element_type=jnp.float32)
    return total


def from_behind(x, axis, by):
    length = lax.axis_size(axis)
    pairs = [(i, i + by) for i in range(length) if 0 <= i + by < length]
    return lax.ppermute(x, axis, pairs)


def root_norm(values, gain):
    values = values.astype(jnp.float32)
    return values * lax.rsqrt(jnp.mean(values * values, axis=-1, keepdims=True) + 1e-06) * gain


def rotate_halves(values, token_positions):
    row_count = values.shape[0]
    shaped = values.reshape(row_count, -1, HEAD_SIZE)
    half_dim = HEAD_SIZE // 2
    freq = 10000.0 ** (-(jnp.arange(half_dim).astype(jnp.float32) * 2.0 / HEAD_SIZE))
    angle = token_positions[:, None] * freq[None, :]
    cosine = jnp.cos(angle)[:, None, :]
    sine_part = jnp.sin(angle)[:, None, :]
    first = shaped[..., :half_dim]
    second = shaped[..., half_dim:]
    turned = jnp.concatenate(
        [first * cosine - second * sine_part, second * cosine + first * sine_part], axis=-1
    )
    return turned.reshape(row_count, -1)


def attend(query_rows, keys_now, vals_now, keys_prior, vals_prior, offset_pos):
    length = query_rows.shape[0]
    kv_heads = keys_now.shape[1] // HEAD_SIZE
    repeat_heads = query_rows.shape[1] // (HEAD_SIZE * kv_heads)
    query_grouped = query_rows.reshape(length, kv_heads, repeat_heads, HEAD_SIZE)
    key_current = jnp.concatenate([keys_prior, keys_now], axis=0).reshape(
        2 * length, kv_heads, HEAD_SIZE
    )
    value_current = jnp.concatenate([vals_prior, vals_now], axis=0).reshape(
        2 * length, kv_heads, HEAD_SIZE
    )
    attention_scores = jnp.einsum(
        "cwap,bwp->wacb", query_grouped, key_current, preferred_element_type=jnp.float32
    )
    query_idx = jnp.arange(length)[:, None]
    key_idx = jnp.arange(2 * length)[None, :]
    key_pos = offset_pos - length + key_idx
    allowed = (key_idx > query_idx) & (key_idx <= query_idx + length) & (key_pos >= 0)
    weights = jnp.where(allowed, jnp.exp(attention_scores), 0.0)
    denominator = jnp.sum(weights, axis=-1)
    weight_narrow = weights.astype(jnp.bfloat16)
    reduced_output = jnp.einsum(
        "bpqu,ubm->qbpm", weight_narrow, value_current, preferred_element_type=jnp.float32
    )
    attended = reduced_output / jnp.transpose(denominator, (2, 0, 1))[..., None]
    return attended.astype(jnp.bfloat16).reshape(length, -1)


def local(tokens, pre_gain, post_gain, w_query, key_matrix, value_matrix, w_out):
    normalized_input = root_norm(tokens, pre_gain).astype(jnp.bfloat16)
    query_cols = w_query.shape[1]
    key_cols = key_matrix.shape[1]
    slab = jnp.concatenate([w_query, key_matrix, value_matrix], axis=1)
    out_full = w_out_of_heads(w_out.T)
    piece = to_every_tp(in_ring_order(normalized_input)).reshape(-1, normalized_input.shape[1])
    joined = times_ring_weights(piece, slab)
    raw_q = joined[:, :query_cols]
    raw_k = joined[:, query_cols : query_cols + key_cols]
    raw_v = joined[:, query_cols + key_cols :]
    offset_pos = lax.axis_index(SEQ) * BLOCK_TOKENS
    token_positions = (offset_pos + jnp.arange(BLOCK_TOKENS)).astype(jnp.float32)
    query_rows = (rotate_halves(raw_q, token_positions) * HEAD_SIZE ** (-0.5)).astype(jnp.bfloat16)
    keys_now = rotate_halves(raw_k, token_positions).astype(jnp.bfloat16)
    vals_now = raw_v.astype(jnp.bfloat16)
    keys_prior, vals_prior = from_behind((keys_now, vals_now), SEQ, 1)
    attended = attend(query_rows, keys_now, vals_now, keys_prior, vals_prior, offset_pos)
    partial_value = lax.dot_general(
        attended, out_full, (((1,), (1,)), ((), ())), preferred_element_type=jnp.float32
    )
    length = lax.axis_size(TP)
    pieces = partial_value.astype(jnp.bfloat16).reshape(length, -1, partial_value.shape[1])
    received = lax.all_to_all(pieces, TP, 0, 0, tiled=True)
    own_rows = jnp.sum(received.astype(jnp.float32), axis=0)
    mixed = root_norm(own_rows, post_gain)
    return (tokens.astype(jnp.float32) + mixed).astype(jnp.bfloat16)


def solution(mesh):
    finer = Mesh(mesh.devices.reshape(16, 2, 2, 2, 4), ("seq_0", "seq_1", "seq_2", "tp_0", "tp_1"))
    in_specs = (P(SEQ_TP, None), P(), P(), P(SEQ, TP), P(SEQ, TP), P(SEQ, TP), P(TP, SEQ))
    out_specs = P(SEQ_TP, None)
    return jax.shard_map(local, mesh=finer, in_specs=in_specs, out_specs=out_specs, check_vma=False)
```

```python
import jax
import jax.numpy as jnp
from jax import lax
from jax.experimental import pallas as pl
from jax.experimental.pallas import tpu as pltpu
from jax.sharding import Mesh
from jax.sharding import PartitionSpec as P

HEAD_SIZE = 256
BLOCK_TOKENS = 512
SEQ = ("seq_0", "seq_1", "seq_2")
TP = ("tp_0", "tp_1")
SEQ_TP = ("seq_0", "seq_1", "seq_2", "tp_0", "tp_1")


def to_every_tp(x):
    length = lax.axis_size(TP)
    return lax.all_to_all(jnp.broadcast_to(x[None], (length, *x.shape)), TP, 0, 0, tiled=True)


def weights_of_heads(slab):
    beside = lax.ppermute(slab, "seq_1", [(0, 1), (1, 0)])
    first = lax.axis_index("seq_1") == 0
    both = jnp.concatenate([jnp.where(first, slab, beside), jnp.where(first, beside, slab)], axis=0)
    gathered = lax.all_gather(both, ("seq_0", "seq_2"), axis=0, tiled=True)
    return gathered.reshape(lax.axis_size("seq_0"), 2, 2, *slab.shape)


def from_behind(x, axis, by):
    length = lax.axis_size(axis)
    pairs = [(i, i + by) for i in range(length) if 0 <= i + by < length]
    return lax.ppermute(x, axis, pairs)


def root_norm(values, gain):
    values = values.astype(jnp.float32)
    return values * lax.rsqrt(jnp.mean(values * values, axis=-1, keepdims=True) + 1e-06) * gain


CHUNKS = 4


def angles(token_positions):
    half_dim = HEAD_SIZE // 2
    freq = 10000.0 ** (-(jnp.arange(half_dim).astype(jnp.float32) * 2.0 / HEAD_SIZE))
    angle = token_positions[:, None] * freq[None, :]
    return jnp.cos(angle), jnp.sin(angle)


def weight_copies(w_hbm, w_vmem, sems, column, depths):
    rows, width = w_hbm.shape[3], w_vmem.shape[1]
    each = depths // CHUNKS
    copies = []
    for chunk in range(CHUNKS):
        for z in range(chunk * each, (chunk + 1) * each):
            for core in range(2):
                for chip in range(2):
                    at = ((z * 2 + chip) * 2 + core) * rows
                    copies.append(
                        pltpu.make_async_copy(
                            w_hbm.at[z, core, chip, :, pl.ds(column, width)],
                            w_vmem.at[pl.ds(at, rows), :],
                            sems.at[len(copies)],
                        )
                    )
    return copies


def turned(values, cosine, sine):
    half = HEAD_SIZE // 2
    first, second = values[:, :half], values[:, half:]
    return jnp.concatenate([first * cosine - second * sine, second * cosine + first * sine], axis=1)


def projected(x_hbm, w_hbm, x_vmem, w_vmem, x_sems, w_sems, column):
    copies = weight_copies(w_hbm, w_vmem, w_sems, column, w_hbm.shape[0])
    per = len(copies) // CHUNKS
    depth = x_vmem.shape[1] // CHUNKS
    x_copies = [
        pltpu.make_async_copy(
            x_hbm.at[:, pl.ds(k * depth, depth)], x_vmem.at[:, pl.ds(k * depth, depth)], x_sems.at[k]
        )
        for k in range(CHUNKS)
    ]
    for k in range(CHUNKS):
        x_copies[k].start()
        for copy in copies[k * per : (k + 1) * per]:
            copy.start()
    total = None
    for k in range(CHUNKS):
        x_copies[k].wait()
        for copy in copies[k * per : (k + 1) * per]:
            copy.wait()
        part = jnp.dot(
            x_vmem[:, k * depth : (k + 1) * depth],
            w_vmem[k * depth : (k + 1) * depth, :],
            preferred_element_type=jnp.float32,
        )
        total = part if total is None else total + part
    return total


def kv_kernel(x_hbm, w_hbm, cos_ref, sin_ref, out_ref, x_vmem, w_vmem, x_sems, w_sems, *, column):
    total = projected(x_hbm, w_hbm, x_vmem, w_vmem, x_sems, w_sems, column)
    out_ref[:, :HEAD_SIZE] = turned(total[:, :HEAD_SIZE], cos_ref[...], sin_ref[...]).astype(jnp.bfloat16)
    out_ref[:, HEAD_SIZE:] = total[:, HEAD_SIZE:].astype(jnp.bfloat16)


def q_kernel(x_hbm, w_hbm, cos_ref, sin_ref, out_ref, x_vmem, w_vmem, x_sems, w_sems, *, column):
    total = projected(x_hbm, w_hbm, x_vmem, w_vmem, x_sems, w_sems, column)
    for head in range(total.shape[1] // HEAD_SIZE):
        part = slice(head * HEAD_SIZE, (head + 1) * HEAD_SIZE)
        rotated = turned(total[:, part], cos_ref[...], sin_ref[...])
        out_ref[:, part] = (rotated * HEAD_SIZE ** (-0.5)).astype(jnp.bfloat16)


def projection(kernel, piece, gathered, cosine, sine, column, width):
    rows, depth = piece.shape
    copies = gathered.shape[0] * 4
    anywhere, inside = pl.BlockSpec(memory_space=pl.ANY), pl.BlockSpec(memory_space=pltpu.VMEM)
    return pl.pallas_call(
        lambda *refs: kernel(*refs, column=column),
        out_shape=jax.ShapeDtypeStruct((rows, width), jnp.bfloat16),
        in_specs=[anywhere, anywhere, inside, inside],
        out_specs=inside,
        scratch_shapes=[
            pltpu.VMEM((rows, depth), jnp.bfloat16),
            pltpu.VMEM((depth, width), jnp.bfloat16),
            pltpu.SemaphoreType.DMA((CHUNKS,)),
            pltpu.SemaphoreType.DMA((copies,)),
        ],
        cost_estimate=pl.CostEstimate(
            flops=2 * rows * depth * width, transcendentals=0, bytes_accessed=2 * depth * (rows + width)
        ),
        name=kernel.__name__,
    )(piece, gathered, cosine, sine)


TILE = 128


def attend_kernel(least_ref, q_ref, now_ref, prior_ref, w_hbm, out_hbm, keys, held, w_vmem, made, w_sems, out_sems, *, column):
    copies = weight_copies(w_hbm, w_vmem, w_sems, column, w_hbm.shape[0])
    for copy in copies:
        copy.start()
    length = q_ref.shape[0]
    heads = q_ref.shape[1] // HEAD_SIZE
    keys[:length, :] = prior_ref[...]
    keys[length:, :] = now_ref[...]
    span = length + TILE
    row = lax.broadcasted_iota(jnp.int32, (heads, TILE, span), 1).reshape(heads * TILE, span)
    column_at = lax.broadcasted_iota(jnp.int32, (heads * TILE, span), 1)
    window = (column_at > row) & (column_at <= row + length)
    for t in range(length // TILE):
        at = t * TILE
        q = jnp.concatenate(
            [q_ref[at : at + TILE, h * HEAD_SIZE : (h + 1) * HEAD_SIZE] for h in range(heads)], axis=0
        )
        scores = lax.dot_general(
            q, keys[at : at + span, :HEAD_SIZE], (((1,), (1,)), ((), ())), preferred_element_type=jnp.float32
        )
        seen = window & (column_at + at >= least_ref[0])
        weights = jnp.where(seen, jnp.exp(scores), 0.0)
        denom = jnp.sum(weights, axis=1, keepdims=True)
        reduced = jnp.dot(
            weights.astype(jnp.bfloat16), keys[at : at + span, HEAD_SIZE:], preferred_element_type=jnp.float32
        )
        reduced = (reduced / denom).astype(jnp.bfloat16)
        for h in range(heads):
            held[at : at + TILE, h * HEAD_SIZE : (h + 1) * HEAD_SIZE] = reduced[h * TILE : (h + 1) * TILE]
    per = len(copies) // CHUNKS
    width = w_vmem.shape[0] // CHUNKS
    sends = []
    for k in range(CHUNKS):
        for copy in copies[k * per : (k + 1) * per]:
            copy.wait()
        part = pl.ds(k * width, width)
        made[:, part] = lax.dot_general(
            held[...], w_vmem[part, :], (((1,), (1,)), ((), ())), preferred_element_type=jnp.float32
        ).astype(jnp.bfloat16)
        sends.append(pltpu.make_async_copy(made.at[:, part], out_hbm.at[:, part], out_sems.at[k]))
        sends[-1].start()
    for send in sends:
        send.wait()


def attended_out(queries, now, prior, gathered, least, column):
    length, width = queries.shape
    depth = gathered.shape[0] * 4 * gathered.shape[3]
    anywhere, inside = pl.BlockSpec(memory_space=pl.ANY), pl.BlockSpec(memory_space=pltpu.VMEM)
    return pl.pallas_call(
        lambda *refs: attend_kernel(*refs, column=column),
        out_shape=jax.ShapeDtypeStruct((length, depth), jnp.bfloat16),
        in_specs=[pl.BlockSpec(memory_space=pltpu.SMEM), inside, inside, inside, anywhere],
        out_specs=anywhere,
        scratch_shapes=[
            pltpu.VMEM((2 * length, 2 * HEAD_SIZE), jnp.bfloat16),
            pltpu.VMEM((length, width), jnp.bfloat16),
            pltpu.VMEM((depth, width), jnp.bfloat16),
            pltpu.VMEM((length, depth), jnp.bfloat16),
            pltpu.SemaphoreType.DMA((gathered.shape[0] * 4,)),
            pltpu.SemaphoreType.DMA((CHUNKS,)),
        ],
        cost_estimate=pl.CostEstimate(
            flops=2 * length * width * (depth + 4 * length), transcendentals=2 * length * length, bytes_accessed=4 * depth * width
        ),
        name="attend_kernel",
    )(least, queries, now, prior, gathered)


def local(tokens, pre_gain, post_gain, w_query, key_matrix, value_matrix, w_out):
    normalized_input = root_norm(tokens, pre_gain).astype(jnp.bfloat16)
    query_cols = w_query.shape[1]
    key_cols = key_matrix.shape[1]
    slab = jnp.concatenate([w_query, key_matrix, value_matrix, w_out.T], axis=1)
    gathered = weights_of_heads(slab)
    width = query_cols + 2 * key_cols
    piece = to_every_tp(normalized_input).reshape(-1, normalized_input.shape[1])
    offset_pos = lax.axis_index(SEQ) * BLOCK_TOKENS
    cosine, sine = angles((offset_pos + jnp.arange(BLOCK_TOKENS)).astype(jnp.float32))
    now = projection(kv_kernel, piece, gathered, cosine, sine, query_cols, 2 * key_cols)
    prior = from_behind(now, SEQ, 1)
    queries = projection(q_kernel, piece, gathered, cosine, sine, 0, query_cols)
    least = jnp.where(offset_pos > 0, 0, BLOCK_TOKENS).astype(jnp.int32).reshape(1)
    partial_value = attended_out(queries, now, prior, gathered, least, width)
    length = lax.axis_size(TP)
    pieces = partial_value.reshape(length, -1, partial_value.shape[1])
    received = lax.all_to_all(pieces, TP, 0, 0, tiled=True)
    own_rows = jnp.sum(received.astype(jnp.float32), axis=0)
    mixed = root_norm(own_rows, post_gain)
    return (tokens.astype(jnp.float32) + mixed).astype(jnp.bfloat16)


def solution(mesh):
    finer = Mesh(mesh.devices.reshape(16, 2, 2, 2, 4), ("seq_0", "seq_1", "seq_2", "tp_0", "tp_1"))
    in_specs = (P(SEQ_TP, None), P(), P(), P(SEQ, TP), P(SEQ, TP), P(SEQ, TP), P(TP, SEQ))
    out_specs = P(SEQ_TP, None)
    return jax.shard_map(local, mesh=finer, in_specs=in_specs, out_specs=out_specs, check_vma=False)
```
